128 devices in a mesh: grp: 4 (over y), dev: 32 (over z, x, core).
Axes of the slice: x: 4, y: 4, z: 4, core: 2. Of those that a mesh axis runs over, the one named last changes fastest.
Arguments:
- examples: float32 [8192, 32768], P(('grp', 'dev'))
- labels: int32 [8192], P(('grp', 'dev')), may hold values from 0 to 1, as said below
Outputs:
- consensus: float32 [32768], replicated
- local_weights: float32 [128, 32768], P(('grp', 'dev'))
- dual_vars: float32 [128, 32768], P(('grp', 'dev'))
The draws below stay inside these ranges and needn't reach their ends.
Inputs may be any that keep to these rules, and one draw needn't show every extreme that they name: `labels`: each example's class, 0 or 1.
All inputs are finite; a program needn't handle non-finite values.
Results may differ from the reference program's by a relative error of at most 0.00012.
Values sent between devices are 32-bit elements; how exact they have to be, the bound alone decides.
A program may use at most 64 MiB of HBM per device.

```python
import jax
import jax.numpy as jnp
from jax import lax

F = 32768
ROWS = 64
PROX = 3
ROUNDS = 4
TOTAL_ROWS = 8192
N_GRP = 4
N_DEV = 32


def label_keys(key):
    base = jax.random.fold_in(key, 7)
    label_key, noise_key, direction_random_key = jax.random.split(base, 3)
    classes = jax.random.randint(label_key, (TOTAL_ROWS,), 0, 2).astype(jnp.int32)
    return (classes, noise_key, direction_random_key)


def draw_labels(key, part):
    classes, noise_key, direction_random_key = label_keys(key)
    return classes


def draw_examples(key, part):
    classes, noise_key, direction_random_key = label_keys(key)
    direction = jax.random.normal(direction_random_key, (F,), jnp.float32)
    polarity = 2.0 * classes.astype(jnp.float32) - 1.0
    strength = 0.6 / jnp.sqrt(jnp.float32(ROWS))
    noise_part = jax.random.normal(noise_key, (TOTAL_ROWS, F), jnp.float32)
    values = noise_part + strength * polarity[:, None] * direction[None, :]
    values = values / (10.0 * jnp.sqrt(jnp.float32(F)))
    return values.astype(jnp.float32)


def setup_inputs(seed: int = 0) -> dict:
    key_list = jax.random.split(jax.random.key(seed), 3)
    return {
        "examples": draw_examples(jax.random.fold_in(key_list[2], 71), 0),
        "labels": draw_labels(jax.random.fold_in(key_list[2], 71), 0),
    }


step_size = 200.0
penalty = 0.005
thresh = 0.04


def shrink(values):
    return values - jnp.clip(values, -thresh, thresh)


def reference(examples, labels):
    members = N_GRP * N_DEV
    example_blocks = examples.reshape(members, ROWS, F)
    targets = labels.reshape(members, ROWS).astype(jnp.float32)

    def one_round(round_index, carried):
        consensus, weight_vector, dual_vars = carried
        consensus_point = consensus[None, :] - dual_vars
        for prox_index in range(PROX):
            label_margins = jnp.einsum("guz,gz->gu", example_blocks, weight_vector, precision=lax.Precision.HIGHEST)
            primal_residual = jax.nn.sigmoid(label_margins) - targets
            loss_gradient = jnp.einsum("pjl,pj->pl", example_blocks, primal_residual, precision=lax.Precision.HIGHEST)
            weight_vector = (weight_vector - step_size * loss_gradient + step_size * penalty * consensus_point) / (1.0 + step_size * penalty)
        average = jnp.sum(weight_vector + dual_vars, axis=0) / members
        consensus = shrink(average)
        dual_vars = dual_vars + weight_vector - consensus[None, :]
        return consensus, weight_vector, dual_vars

    start = (jnp.zeros((F,), jnp.float32), jnp.zeros((members, F), jnp.float32), jnp.zeros((members, F), jnp.float32))
    consensus, weight_vector, dual_vars = lax.fori_loop(0, ROUNDS, one_round, start)
    return consensus, weight_vector, dual_vars
```

```python
import jax
import jax.numpy as jnp
from jax import lax
from jax.experimental import pallas as pl
from jax.experimental.pallas import tpu as pltpu
from jax.sharding import PartitionSpec as P

PROX = 3
ROUNDS = 4
THRESH = 0.04
STEP = 200.0
PENALTY = 0.005
MESH = pl.DeviceIdType.MESH
CHUNKS = 8
BF16 = jnp.bfloat16
F32 = jnp.float32

ORDER = (2, 1, 3, 0)
PEERS = sorted(
    [
        (dy, dz, dx, dc)
        for dy in ORDER
        for dz in ORDER
        for dx in ORDER
        for dc in (1, 0)
        if (dy, dz, dx, dc) != (0, 0, 0, 0)
    ],
    key=lambda o: -sum(min(d, 4 - d) for d in o[:3]),
)


def kernel(rows, feats, n, labels_ref, x_hbm, z_ref, w_ref, u_ref, xv, gram, h, rs, zb, zmine, x_sems, send_rs, recv_rs, send_ag, recv_ag):
    grp = lax.axis_index("grp")
    dev = lax.axis_index("dev")
    me = grp * 32 + dev
    core = lax.rem(dev, 2)
    px = lax.rem(lax.div(dev, 2), 4)
    pz = lax.div(dev, 8)
    width = feats // CHUNKS

    def copy_in(c):
        cols = pl.ds(c * width, width)
        return pltpu.make_async_copy(x_hbm.at[:, cols], xv.at[:, cols], x_sems.at[c])

    for c in range(CHUNKS):
        copy_in(c).start()

    ys = [lax.rem(grp + d, 4) for d in range(4)]
    zs = [lax.rem(pz + d, 4) * 8 for d in range(4)]
    xs = [lax.rem(px + d, 4) * 2 for d in range(4)]
    cs = [core, 1 - core]

    def peer(offset):
        dy, dz, dx, dc = offset
        ty = ys[dy]
        td = zs[dz] + xs[dx] + cs[dc]
        return ty, td

    barrier = pltpu.get_barrier_semaphore()
    for offset in PEERS:
        pl.semaphore_signal(barrier, inc=1, device_id=peer(offset), device_id_type=MESH)

    sub = 512
    acc = jnp.zeros((2 * rows, rows), F32)
    for c in range(CHUNKS):
        copy_in(c).wait()

        def gram_step(i, acc, c=c):
            xs_ = xv[:, pl.ds(pl.multiple_of(c * width + i * sub, sub), sub)]
            hi = xs_.astype(BF16)
            lo = (xs_ - hi.astype(F32)).astype(BF16)
            both = jnp.concatenate([hi, lo], axis=0)
            return acc + lax.dot_general(both, hi, (((1,), (1,)), ((), ())), preferred_element_type=F32)

        acc = lax.fori_loop(0, width // sub, gram_step, acc)
    cross = acc[rows:]
    gram[...] = acc[:rows] + cross + cross.T

    r_i = lax.broadcasted_iota(jnp.int32, (rows, rows), 0)
    c_i = lax.broadcasted_iota(jnp.int32, (rows, rows), 1)
    eye = r_i == c_i
    targets = jnp.sum(jnp.where(eye, labels_ref[...].astype(F32), 0.0), axis=1, keepdims=True)

    w_ref[...] = jnp.zeros_like(w_ref)
    u_ref[...] = jnp.zeros_like(u_ref)
    zb[...] = jnp.zeros_like(zb)

    pl.semaphore_wait(barrier, n - 1)

    def gram_times(r):
        r_row = jnp.sum(jnp.where(eye, r, 0.0), axis=0, keepdims=True)
        return jnp.sum(gram[...] * r_row, axis=1, keepdims=True)

    def one_round(k, carried):
        m, xu, xz, mean_w, mean_u, z_own = carried
        par = lax.rem(k, 2)
        prev = 1 - par
        q = xz - xu
        total = jnp.zeros((rows, 1), F32)
        for t in range(PROX):
            r = jax.nn.sigmoid(m) - targets
            total = 0.5 * total + r
            m = 0.5 * (m + q) - (STEP * 0.5) * gram_times(r)
        scaled = jnp.broadcast_to((-STEP * 0.5) * total, (rows, 128))

        def back(j, _):
            for half in range(2):
                cols = pl.ds(pl.multiple_of(j * 256 + half * 128, 128), 128)
                h[j, half : half + 1, :] = jnp.sum(xv[:, cols] * scaled, axis=0, keepdims=True)
            return 0

        lax.fori_loop(0, n, back, 0, unroll=4)

        for offset in PEERS:
            ty, td = peer(offset)
            pltpu.make_async_remote_copy(
                src_ref=h.at[ty * 32 + td],
                dst_ref=rs.at[me],
                send_sem=send_rs,
                recv_sem=recv_rs,
                device_id=(ty, td),
                device_id_type=MESH,
            ).start()
        rs[me] = h[me]
        u = u_ref[...] + jnp.where(k > 0, 1.0, 0.0) * (w_ref[...] - zb[prev])
        u_ref[...] = u
        w_ref[...] = 0.125 * w_ref[...] + 0.875 * (zb[prev] - u) + h[...]

        some = rs.at[pl.ds(0, n - 1)]
        waiter = pltpu.make_async_remote_copy(
            src_ref=some, dst_ref=some, send_sem=send_rs, recv_sem=recv_rs, device_id=(grp, dev), device_id_type=MESH
        )
        waiter.wait_recv()
        mean_h = jnp.sum(rs[...], axis=0) * (1.0 / n)
        new_mean_w = 0.125 * mean_w + 0.875 * (z_own - mean_u) + mean_h
        a = new_mean_w + mean_u
        z_new = a - jnp.clip(a, -THRESH, THRESH)
        zmine[...] = z_new
        for offset in PEERS:
            ty, td = peer(offset)
            pltpu.make_async_remote_copy(
                src_ref=zmine,
                dst_ref=zb.at[par, me],
                send_sem=send_ag,
                recv_sem=recv_ag,
                device_id=(ty, td),
                device_id_type=MESH,
            ).start()
        zb[par, me] = z_new
        waiter.wait_send()
        got = zb.at[par, pl.ds(0, n - 1)]
        waiter_ag = pltpu.make_async_remote_copy(
            src_ref=got, dst_ref=got, send_sem=send_ag, recv_sem=recv_ag, device_id=(grp, dev), device_id_type=MESH
        )
        waiter_ag.wait_recv()

        def fwd(j, acc):
            for half in range(2):
                cols = pl.ds(pl.multiple_of(j * 256 + half * 128, 128), 128)
                acc = acc + xv[:, cols] * zb[par, j, half : half + 1, :]
            return acc

        acc = lax.fori_loop(0, n, fwd, jnp.zeros((rows, 128), F32), unroll=4)
        new_xz = jnp.sum(acc, axis=1, keepdims=True)
        waiter_ag.wait_send()
        xu = xu + m - new_xz
        return m, xu, new_xz, new_mean_w, a - z_new, z_new

    col = jnp.zeros((rows, 1), F32)
    piece = jnp.zeros((2, 128), F32)
    lax.fori_loop(0, ROUNDS, one_round, (col, col, col, piece, piece, piece))
    last = (ROUNDS - 1) % 2
    z_ref[...] = zb[last]
    u_ref[...] = u_ref[...] + w_ref[...] - zb[last]


def solution(mesh):
    n = mesh.size

    def per_device(examples, labels):
        rows, feats = examples.shape
        import functools

        vec = jax.ShapeDtypeStruct((n, 2, 128), F32)
        vmem = pl.BlockSpec(memory_space=pltpu.VMEM)
        z, w, u = pl.pallas_call(
            functools.partial(kernel, rows, feats, n),
            out_shape=(vec, vec, vec),
            in_specs=[vmem, pl.BlockSpec(memory_space=pl.ANY)],
            out_specs=(vmem, vmem, vmem),
            scratch_shapes=[
                pltpu.VMEM((rows, feats), F32),
                pltpu.VMEM((rows, rows), F32),
                pltpu.VMEM((n, 2, 128), F32),
                pltpu.VMEM((n, 2, 128), F32),
                pltpu.VMEM((2, n, 2, 128), F32),
                pltpu.VMEM((2, 128), F32),
                pltpu.SemaphoreType.DMA((CHUNKS,)),
                pltpu.SemaphoreType.DMA,
                pltpu.SemaphoreType.DMA,
                pltpu.SemaphoreType.DMA,
                pltpu.SemaphoreType.DMA,
            ],
            compiler_params=pltpu.CompilerParams(collective_id=0, has_side_effects=True),
        )(labels.reshape(1, rows), examples)
        return z.reshape(feats), w.reshape(1, feats), u.reshape(1, feats)

    return jax.shard_map(
        per_device,
        mesh=mesh,
        in_specs=(P(("grp", "dev"), None), P(("grp", "dev"))),
        out_specs=(P(), P(("grp", "dev"), None), P(("grp", "dev"), None)),
        check_vma=False,
    )
```
